32 devices in a mesh: groups: 2 (over x), seq: 16 (over z, y, core).
Axes of the slice: x: 2, y: 2, z: 4, core: 2. Of those that a mesh axis runs over, the one named last changes fastest.
Arguments:
- query_rows: bfloat16 [16384, 1536], P(('groups', 'seq')), parts along dimension 0, may hold values from -200 to 200
- key_rows: bfloat16 [16384, 1536], P(('groups', 'seq')), parts along dimension 0, may hold values from -6 to 6
- value_rows: bfloat16 [16384, 1536], P(('groups', 'seq')), parts along dimension 0, may hold values from -6 to 6
- select: int32 [64, 6], P('groups'), parts along dimension 0, may hold values from 0 to 31, as said below
- counts: int32 [64], P('groups'), parts along dimension 0, may hold values from 2 to 6, as said below
- guide_scale: float32 [2], P('groups'), parts along dimension 0, may hold values from 4 to 8
Outputs:
- guided: bfloat16 [8192, 1536], P(('groups', 'seq')), parts along dimension 0
The draws below stay inside these ranges and needn't reach their ends.
There are 2 independent parts, one for each index of `groups`. The reference program is written for one: setup_inputs(seed, part) draws one part's arguments, and reference() takes and returns one part's arrays. A program takes and returns all parts, laid end to end along the dimension named above; each array names one. Nothing has to cross between parts.
Inputs may be any that keep to these rules, and one draw needn't show every extreme that they name: Row i begins with i itself. Its first counts[i] entries are distinct and name tiles of shards within 2 of tile i's shard, where tile t belongs to shard t // 4. The query tiles of one shard select at most 2 distinct tiles of any one other shard, and every shard selects 2 tiles of each shard within 2 in every draw. Entries past counts[i] are valid tile numbers that are not used. `counts`: whole shards are heavy or light, so the work of one device differs by about two times between devices.
All inputs are finite; a program needn't handle non-finite values.
Results may differ from the reference program's by a relative error of at most 0.0075.
Values may be sent and summed in bfloat16 or wider, within the bound.
A program may use at most 128 MiB of HBM per device.

```python
import jax
import jax.numpy as jnp
from jax import lax

HEADS = 12
HEAD_DIM = 128
TILE = 128
TOK_DEV = 512
REACH = 2
CAP = 2
PICKS = 6
WIDTH = 1536
TILES_DEV = 4
SHARDS = 8
SEQLEN = 4096
NTILES = 32


def mask_tables(key):
    folded = jax.random.fold_in(key, 101)
    key_pool, key_score, key_heavy, key_count = jax.random.split(folded, 4)
    cand_count = TILES_DEV + 2 * REACH * CAP
    offset_list = jnp.array([moved for moved in range(-REACH, REACH + 1) if moved != 0], dtype=jnp.int32)
    shard_ids = jnp.arange(SHARDS, dtype=jnp.int32)
    tile_ids = jnp.arange(TILES_DEV, dtype=jnp.int32)
    pool_scores = jax.random.randint(key_pool, (SHARDS, 2 * REACH, TILES_DEV), 0, 1 << 16, dtype=jnp.int32) * TILES_DEV + tile_ids
    pool_local = lax.top_k(pool_scores, CAP)[1].astype(jnp.int32)
    owner_ids = shard_ids[:, None, None] + offset_list[None, :, None]
    pool_tiles = owner_ids * TILES_DEV + pool_local
    pool_valid = jnp.broadcast_to((owner_ids >= 0) & (owner_ids < SHARDS), pool_local.shape)
    local_tiles = shard_ids[:, None] * TILES_DEV + tile_ids[None, :]
    candidates = jnp.concatenate([local_tiles, pool_tiles.reshape(SHARDS, 2 * REACH * CAP)], axis=1)
    cand_valid = jnp.concatenate([jnp.ones((SHARDS, TILES_DEV), dtype=bool), pool_valid.reshape(SHARDS, 2 * REACH * CAP)], axis=1)
    cand_index = jnp.arange(cand_count, dtype=jnp.int32)
    noise_scores = jax.random.randint(key_score, (SHARDS, TILES_DEV, cand_count), 0, 1 << 16, dtype=jnp.int32) * cand_count + cand_index
    self_slot = cand_index[None, :] == tile_ids[:, None]
    block_index = (cand_index - TILES_DEV) // CAP
    row_of_block = (shard_ids[:, None] + block_index[None, :]) % TILES_DEV
    in_forced = (cand_index >= TILES_DEV)[None, None, :] & (tile_ids[None, :, None] == row_of_block[:, None, :])
    total_score = noise_scores + jnp.where(self_slot[None, :, :], 1 << 26, 0) + jnp.where(in_forced, 1 << 24, 0) - jnp.where(cand_valid[:, None, :], 0, 1 << 27)
    best_index = lax.top_k(total_score, PICKS)[1].astype(jnp.int32)
    spread = jnp.broadcast_to(candidates[:, None, :], (SHARDS, TILES_DEV, cand_count))
    select = jnp.take_along_axis(spread, best_index, axis=2).reshape(NTILES, PICKS).astype(jnp.int32)
    heavy_shard = jax.random.randint(key_heavy, (SHARDS,), 0, 4, dtype=jnp.int32) == 0
    many_picks = jax.random.randint(key_count, (SHARDS, TILES_DEV), PICKS - 2, PICKS + 1, dtype=jnp.int32)
    few_picks = jax.random.randint(jax.random.fold_in(key_count, 3), (SHARDS, TILES_DEV), 2, 4, dtype=jnp.int32)
    counts = jnp.where(heavy_shard[:, None], many_picks, few_picks)
    forced_row = (tile_ids[None, :] - shard_ids[:, None]) % TILES_DEV < 2 * REACH
    counts = jnp.where(forced_row, jnp.maximum(counts, CAP + 1), counts).reshape(NTILES).astype(jnp.int32)
    return (select, counts)


def draw_select(key, part):
    return mask_tables(key)[0]


def draw_counts(key, part):
    return mask_tables(key)[1]


def query_key_tables(key):
    folded = jax.random.fold_in(key, 202)
    key_query, key_key = jax.random.split(folded, 2)
    queries = jax.random.normal(key_query, (2 * SEQLEN, HEADS, HEAD_DIM), jnp.float32)
    keyset = jnp.clip(jax.random.normal(key_key, (2 * SEQLEN, HEADS, HEAD_DIM), jnp.float32), -6.0, 6.0)
    queries = jnp.clip(queries, -200.0, 200.0)
    return (queries.reshape(2 * SEQLEN, HEADS * HEAD_DIM), keyset.reshape(2 * SEQLEN, HEADS * HEAD_DIM))


def draw_query_rows(key, part):
    return query_key_tables(key)[0].astype(jnp.bfloat16)


def draw_key_rows(key, part):
    return query_key_tables(key)[1].astype(jnp.bfloat16)


def shard_levels(own_key, dims, cuts, low, largest):
    def one(dim, shards_of):
        draws = jax.random.uniform(jax.random.fold_in(jax.random.fold_in(own_key, 6), dim), (shards_of,), jnp.float32, low / len(cuts), largest / len(cuts))
        return jnp.repeat(jnp.exp(draws), dims[dim] // shards_of).reshape((-1,) + (1,) * (len(dims) - dim - 1))

    factor_of = one(*cuts[0])
    for cut in cuts[1:]:
        factor_of = factor_of * one(*cut)
    return factor_of


def scatter_about(own_key, dims, deviation, most, shards=(), kind=jnp.bfloat16):
    drawn = deviation * jax.random.normal(own_key, dims, jnp.float32)
    if shards:
        drawn = drawn * shard_levels(own_key, dims, shards, -0.22, 0.18)
    return jnp.clip(drawn, -most, most).astype(kind)


def setup_inputs(seed: int = 0, part: int = 0) -> dict:
    splits = jax.random.split(jax.random.key(seed), 7)
    own_keys = jax.random.split(jax.random.fold_in(splits[6], part), 7)
    query_rows = draw_query_rows(jax.random.fold_in(jax.random.fold_in(splits[6], part), 71), part)
    key_rows = draw_key_rows(jax.random.fold_in(jax.random.fold_in(splits[6], part), 71), part)
    value_rows = scatter_about(own_keys[2], (2 * SEQLEN, WIDTH), 1.0, 6.0, ((0, 16),))
    select = draw_select(jax.random.fold_in(jax.random.fold_in(splits[6], part), 71), part)
    counts = draw_counts(jax.random.fold_in(jax.random.fold_in(splits[6], part), 71), part)
    guide_scale = jnp.clip(jax.random.uniform(own_keys[5], (1,), jnp.float32, 4.0, 8.0), 4.0, 8.0)
    return {"query_rows": query_rows, "key_rows": key_rows, "value_rows": value_rows, "select": select, "counts": counts, "guide_scale": guide_scale}


def attend_tile(query_tile, key_sel, value_sel, alive_slots):
    score_scale = HEAD_DIM ** -0.5
    scores = jnp.einsum("thd,pshd->htps", query_tile.astype(jnp.float32), key_sel.astype(jnp.float32)) * score_scale
    scores = jnp.where(alive_slots[None, None, :, None], scores, -jnp.inf)
    row_max = jnp.max(scores, axis=(2, 3), keepdims=True)
    weights = jnp.exp(scores - row_max)
    denominator = jnp.sum(weights, axis=(2, 3))
    rounded = lax.optimization_barrier(weights.astype(jnp.bfloat16)).astype(jnp.float32)
    weighted = jnp.einsum("htps,pshd->thd", rounded, value_sel.astype(jnp.float32))
    return (weighted / jnp.transpose(denominator)[:, :, None]).astype(jnp.bfloat16)


def branch_major(rows, ntiles):
    split = rows.reshape(SHARDS, 2, TOK_DEV, HEADS * HEAD_DIM)
    return jnp.transpose(split, (1, 0, 2, 3)).reshape(2, ntiles, TILE, HEADS, HEAD_DIM)


def reference(query_rows, key_rows, value_rows, select, counts, guide_scale):
    ntiles = select.shape[0]
    query_tiles = branch_major(query_rows, ntiles)
    key_tiles = branch_major(key_rows, ntiles)
    value_tiles = branch_major(value_rows, ntiles)
    alive_all = jnp.arange(PICKS, dtype=jnp.int32)[None, :] < counts[:, None]
    guidance = guide_scale[0]

    def one_tile(inputs):
        cond_query, uncond_query, chosen, alive_slots = inputs
        cond_out = attend_tile(cond_query, key_tiles[0][chosen], value_tiles[0][chosen], alive_slots)
        uncond = attend_tile(uncond_query, key_tiles[1][chosen], value_tiles[1][chosen], alive_slots)
        cond_wide = lax.optimization_barrier(cond_out).astype(jnp.float32)
        uncond_wide = lax.optimization_barrier(uncond).astype(jnp.float32)
        mixed_out = uncond_wide + guidance * (cond_wide - uncond_wide)
        return mixed_out.astype(jnp.bfloat16).reshape(TILE, HEADS * HEAD_DIM)

    guided = lax.map(one_tile, (query_tiles[0], query_tiles[1], select, alive_all), batch_size=4)
    return guided.reshape(ntiles * TILE, HEADS * HEAD_DIM)
```

```python
import functools
import math

import jax
import jax.numpy as jnp
from jax import lax
from jax.experimental import pallas as pl
from jax.experimental.pallas import tpu as pltpu
from jax.sharding import PartitionSpec as P

HEAD_DIM = 128
TILE = 128
REACH = 2
CAP = 2
OFFSETS = (-1, 1, -2, 2)
GROUP_SHARES = (3, 4, 3, 2)


SMEM = pltpu.SMEM


def shift_route(axis, distance):
    devices = range(lax.axis_size(axis))
    return [(i - distance, i) for i in devices if i - distance in devices]


def partner(block, axis):
    count = lax.axis_size(axis)
    return lax.ppermute(block, axis, [(i, i ^ 1) for i in range(count)])


def wanted_span(select_ref, counts_ref, query_shard, owner_shard, shards, tiles_dev):
    first_row = jnp.clip(query_shard, 0, shards - 1) * tiles_dev
    low, high = jnp.int32(tiles_dev), jnp.int32(-1)
    for row in range(tiles_dev):
        count = counts_ref[first_row + row]
        for pick in range(select_ref.shape[1]):
            local = select_ref[first_row + row, pick] - owner_shard * tiles_dev
            usable = (local >= 0) & (local < tiles_dev) & (pick < count)
            low = jnp.where(usable, jnp.minimum(low, local), low)
            high = jnp.where(usable, jnp.maximum(high, local), high)
    low = jnp.where(high < 0, 0, low)
    return low, jnp.maximum(high, 0)


def meta_kernel(shards, tiles_dev, place_ref, select_ref, counts_ref, send_ref, slots_ref, bias_ref):
    shard = place_ref[0]
    picks = select_ref.shape[1]
    lows = []
    for k, offset in enumerate(OFFSETS):
        low, high = wanted_span(
            select_ref, counts_ref, shard + offset, shard, shards, tiles_dev
        )
        send_ref[CAP * k] = low
        send_ref[CAP * k + 1] = high
        lows.append(
            wanted_span(select_ref, counts_ref, shard, shard - offset, shards, tiles_dev)[0]
        )
    for row in range(tiles_dev):
        count = counts_ref[shard * tiles_dev + row]
        for pick in range(picks):
            local = select_ref[shard * tiles_dev + row, pick] - shard * tiles_dev
            slot = jnp.where((local >= 0) & (local < tiles_dev), local, 0)
            for k, offset in enumerate(OFFSETS):
                away = local + offset * tiles_dev
                there = (away >= 0) & (away < tiles_dev)
                second = jnp.where(away == lows[k], 0, 1)
                slot = jnp.where(there, tiles_dev + CAP * k + second, slot)
            slots_ref[row * picks + pick] = slot
            bias_ref[row * picks + pick] = jnp.where(pick < count, 0.0, -jnp.inf)


def gather_kernel(send_ref, key_ref, value_ref, *out_refs):
    for k, out_ref in enumerate(out_refs):
        for slot in range(CAP):
            rows = pl.ds(pl.multiple_of(send_ref[CAP * k + slot] * TILE, TILE), TILE)
            out_ref[0, slot] = key_ref[rows, :]
            out_ref[1, slot] = value_ref[rows, :]


def attend_kernel(
    tiles_dev, picks, place_ref, slots_ref, bias_ref, query_ref, key_ref, value_ref, *rest
):
    landed = rest[: len(OFFSETS)]
    own_ref, away_ref, pool_k, pool_v = rest[len(OFFSETS) :]
    for tile in range(tiles_dev):
        pool_k[tile] = key_ref[tile * TILE : (tile + 1) * TILE, :]
        pool_v[tile] = value_ref[tile * TILE : (tile + 1) * TILE, :]
    for k, ref in enumerate(landed):
        for slot in range(CAP):
            pool_k[tiles_dev + CAP * k + slot] = ref[0, slot]
            pool_v[tiles_dev + CAP * k + slot] = ref[1, slot]
    half = place_ref[1]
    half_tiles = tiles_dev // 2
    factor = HEAD_DIM**-0.5 * math.log2(math.e)
    for step in range(tiles_dev):
        mine = step >= half_tiles
        side = half if mine else 1 - half
        tile = side * half_tiles + step % half_tiles
        query = query_ref[pl.ds(pl.multiple_of(tile * TILE, TILE), TILE), :]
        slots = [slots_ref[tile * picks + p] for p in range(picks)]
        keys = jnp.concatenate([pool_k[s] for s in slots], axis=0)
        values = jnp.concatenate([pool_v[s] for s in slots], axis=0)
        scores = lax.dot_general(
            query, keys, (((1,), (1,)), ((), ())), preferred_element_type=jnp.float32
        )
        parts = [
            scores[:, p * TILE : (p + 1) * TILE] + bias_ref[tile * picks + p]
            for p in range(picks)
        ]
        top = jnp.max(functools.reduce(jnp.maximum, parts), axis=1, keepdims=True)
        weights = [jnp.exp2((part - top) * factor) for part in parts]
        total = jnp.sum(functools.reduce(jnp.add, weights), axis=1, keepdims=True)
        rounded = jnp.concatenate([w.astype(jnp.bfloat16) for w in weights], axis=1)
        mixed = jnp.dot(rounded, values, preferred_element_type=jnp.float32)
        target = own_ref if mine else away_ref
        rows = slice((step % half_tiles) * TILE, (step % half_tiles + 1) * TILE)
        target[rows, :] = (mixed / total).astype(jnp.bfloat16)


def combine_kernel(starts, place_ref, guide_ref, *refs):
    out_ref = refs[-1]
    first = place_ref[1] == 0
    guidance = guide_ref[0]
    for g, start in enumerate(starts):
        own = refs[2 * g][...].astype(jnp.float32)
        theirs = refs[2 * g + 1][...].astype(jnp.float32)
        cond = jnp.where(first, own, theirs)
        uncond = jnp.where(first, theirs, own)
        guided = uncond + guidance * (cond - uncond)
        out_ref[:, start : start + own.shape[1]] = guided.astype(jnp.bfloat16)


def smem_spec():
    return pl.BlockSpec(memory_space=SMEM)


def head_groups(heads):
    shares = GROUP_SHARES if heads == sum(GROUP_SHARES) else (heads,)
    groups, first = [], 0
    for share in shares:
        groups.append((first, share))
        first += share
    return groups


def body(query_rows, key_rows, value_rows, select, counts, guide_scale):
    shards = lax.axis_size("seq") // 2
    index = lax.axis_index("seq")
    place = jnp.stack([index // 2, index % 2]).astype(jnp.int32)
    tokens, width = query_rows.shape
    tiles_dev = tokens // TILE
    picks = select.shape[1]
    half_rows = tokens // 2
    pool = tiles_dev + CAP * len(OFFSETS)

    send, slots, bias = pl.pallas_call(
        functools.partial(meta_kernel, shards, tiles_dev),
        out_shape=(
            jax.ShapeDtypeStruct((CAP * len(OFFSETS),), jnp.int32),
            jax.ShapeDtypeStruct((tiles_dev * picks,), jnp.int32),
            jax.ShapeDtypeStruct((tiles_dev * picks,), jnp.float32),
        ),
        in_specs=[smem_spec()] * 3,
        out_specs=(smem_spec(),) * 3,
        name="meta",
    )(place, select, counts)

    groups = head_groups(width // HEAD_DIM)
    landed = []
    for first, count in groups:
        cols = count * HEAD_DIM
        source = pl.BlockSpec((tokens, HEAD_DIM), lambda h, first=first: (0, first + h))
        packed = pl.BlockSpec((2, CAP, TILE, HEAD_DIM), lambda h: (0, 0, 0, h))
        outgoing = pl.pallas_call(
            gather_kernel,
            grid=(count,),
            out_shape=[jax.ShapeDtypeStruct((2, CAP, TILE, cols), jnp.bfloat16)] * len(OFFSETS),
            in_specs=[smem_spec(), source, source],
            out_specs=[packed] * len(OFFSETS),
            cost_estimate=pl.CostEstimate(
                flops=0, bytes_accessed=12 * tokens * cols, transcendentals=0
            ),
            name="gather",
        )(send, key_rows, value_rows)
        landed.append(
            [
                lax.ppermute(block, "seq", shift_route("seq", 2 * offset))
                for block, offset in zip(outgoing, OFFSETS)
            ]
        )

    pieces = []
    for (first, count), arrived in zip(groups, landed):
        cols = count * HEAD_DIM
        source = pl.BlockSpec((tokens, HEAD_DIM), lambda h, first=first: (0, first + h))
        packed = pl.BlockSpec((2, CAP, TILE, HEAD_DIM), lambda h: (0, 0, 0, h))
        result = pl.BlockSpec((half_rows, HEAD_DIM), lambda h: (0, h))
        own, away = pl.pallas_call(
            functools.partial(attend_kernel, tiles_dev, picks),
            grid=(count,),
            out_shape=[jax.ShapeDtypeStruct((half_rows, cols), jnp.bfloat16)] * 2,
            in_specs=[smem_spec()] * 3 + [source] * 3 + [packed] * len(OFFSETS),
            out_specs=[result] * 2,
            scratch_shapes=[pltpu.VMEM((pool, TILE, HEAD_DIM), jnp.bfloat16)] * 2,
            cost_estimate=pl.CostEstimate(
                flops=4 * tokens * picks * TILE * cols,
                bytes_accessed=16 * tokens * cols,
                transcendentals=tokens * picks * TILE * count,
            ),
            name="attend",
        )(place, slots, bias, query_rows, key_rows, value_rows, *arrived)
        pieces += [own, partner(away, "seq")]

    starts = [first * HEAD_DIM for first, _ in groups]
    steps = 2
    rows = half_rows // steps
    return pl.pallas_call(
        functools.partial(combine_kernel, starts),
        grid=(steps,),
        out_shape=jax.ShapeDtypeStruct((half_rows, width), jnp.bfloat16),
        in_specs=[smem_spec()] * 2
        + [pl.BlockSpec((rows, piece.shape[1]), lambda r: (r, 0)) for piece in pieces],
        out_specs=pl.BlockSpec((rows, width), lambda r: (r, 0)),
        name="combine",
    )(place, guide_scale, *pieces)


def solution(mesh):
    in_specs = (
        P(("groups", "seq"), None),
        P(("groups", "seq"), None),
        P(("groups", "seq"), None),
        P("groups", None),
        P("groups"),
        P("groups"),
    )
    out_specs = P(("groups", "seq"), None)
    return jax.shard_map(body, mesh=mesh, in_specs=in_specs, out_specs=out_specs, check_vma=False)
```

```python
import functools
import math

import jax
import jax.numpy as jnp
from jax import lax
from jax.experimental import pallas as pl
from jax.experimental.pallas import tpu as pltpu
from jax.sharding import PartitionSpec as P

HEAD_DIM = 128
TILE = 128
REACH = 2
CAP = 2
OFFSETS = (-1, 1, -2, 2)
GROUP_SHARES = (3, 4, 3, 2)

SMEM = pltpu.SMEM


def wanted_span(select_ref, counts_ref, query_shard, owner_shard, shards, tiles_dev):
    first_row = jnp.clip(query_shard, 0, shards - 1) * tiles_dev
    low, high = jnp.int32(tiles_dev), jnp.int32(-1)
    for row in range(tiles_dev):
        count = counts_ref[first_row + row]
        for pick in range(select_ref.shape[1]):
            local = select_ref[first_row + row, pick] - owner_shard * tiles_dev
            usable = (local >= 0) & (local < tiles_dev) & (pick < count)
            low = jnp.where(usable, jnp.minimum(low, local), low)
            high = jnp.where(usable, jnp.maximum(high, local), high)
    low = jnp.where(high < 0, 0, low)
    return low, jnp.maximum(high, 0)


def meta_kernel(shards, tiles_dev, place_ref, select_ref, counts_ref, send_ref, slots_ref, bias_ref):
    shard = place_ref[0]
    picks = select_ref.shape[1]
    lows = []
    for k, offset in enumerate(OFFSETS):
        low, high = wanted_span(
            select_ref, counts_ref, shard + offset, shard, shards, tiles_dev
        )
        send_ref[CAP * k] = low
        send_ref[CAP * k + 1] = high
        lows.append(
            wanted_span(select_ref, counts_ref, shard, shard - offset, shards, tiles_dev)[0]
        )
    for row in range(tiles_dev):
        count = counts_ref[shard * tiles_dev + row]
        for pick in range(picks):
            local = select_ref[shard * tiles_dev + row, pick] - shard * tiles_dev
            slot = jnp.where((local >= 0) & (local < tiles_dev), local, 0)
            for k, offset in enumerate(OFFSETS):
                away = local + offset * tiles_dev
                there = (away >= 0) & (away < tiles_dev)
                second = jnp.where(away == lows[k], 0, 1)
                slot = jnp.where(there, tiles_dev + CAP * k + second, slot)
            slots_ref[row * picks + pick] = slot
            bias_ref[row * picks + pick] = jnp.where(pick < count, 0.0, -jnp.inf)


def main_kernel(groups, tiles_dev, picks, send_ref, slots_ref, bias_ref, guide_ref, *refs):
    query_ref, key_ref, value_ref, out_ref = refs[:4]
    refs = refs[4:]
    pools, outgoing = refs[: len(groups)], refs[len(groups) : 2 * len(groups)]
    own, away, theirs, send_sem, recv_sem, swap_send, swap_recv = refs[2 * len(groups) :]
    index = lax.axis_index("seq")
    shard, half = index // 2, index % 2
    shards = lax.axis_size("seq") // 2
    half_tiles = tiles_dev // 2
    other = index + 1 - 2 * half

    def inside(offset):
        return (shard + offset >= 0) & (shard + offset < shards)

    def route(g, k):
        return pltpu.make_async_remote_copy(
            src_ref=outgoing[g].at[k],
            dst_ref=pools[g].at[pl.ds(tiles_dev + CAP * k, CAP)],
            send_sem=send_sem.at[g, k],
            recv_sem=recv_sem.at[g, k],
            device_id={"seq": index + 2 * OFFSETS[k]},
            device_id_type=pl.DeviceIdType.MESH,
        )

    def swap(g):
        first, count = groups[g]
        cols = pl.ds(first * HEAD_DIM, count * HEAD_DIM)
        return pltpu.make_async_remote_copy(
            src_ref=away.at[:, cols],
            dst_ref=theirs.at[:, cols],
            send_sem=swap_send.at[g],
            recv_sem=swap_recv.at[g],
            device_id={"seq": other},
            device_id_type=pl.DeviceIdType.MESH,
        )

    barrier = pltpu.get_barrier_semaphore()
    pl.semaphore_signal(
        barrier, inc=1, device_id={"seq": other}, device_id_type=pl.DeviceIdType.MESH
    )
    greeted = jnp.int32(1)
    for offset in OFFSETS:
        greeted = greeted + jnp.where(inside(offset), 1, 0)

        @pl.when(inside(offset))
        def _(offset=offset):
            pl.semaphore_signal(
                barrier,
                inc=1,
                device_id={"seq": index + 2 * offset},
                device_id_type=pl.DeviceIdType.MESH,
            )

    def gather(g):
        first, count = groups[g]
        cols = slice(first * HEAD_DIM, (first + count) * HEAD_DIM)
        for k in range(len(OFFSETS)):
            for slot in range(CAP):
                tile = send_ref[CAP * k + slot]
                outgoing[g][k, slot, 0] = key_ref[tile, :, cols]
                outgoing[g][k, slot, 1] = value_ref[tile, :, cols]

    def launch(g):
        for k, offset in enumerate(OFFSETS):

            @pl.when(inside(offset))
            def _(k=k):
                route(g, k).start()

    gather(0)
    pl.semaphore_wait(barrier, greeted)
    for g in range(1, len(groups)):
        gather(g)
        launch(g - 1)
    for g, (first, count) in enumerate(groups):
        cols = slice(first * HEAD_DIM, (first + count) * HEAD_DIM)
        for tile in range(tiles_dev):
            pools[g][tile, 0] = key_ref[tile, :, cols]
            pools[g][tile, 1] = value_ref[tile, :, cols]
        if g == 0:
            launch(len(groups) - 1)

    factor = HEAD_DIM**-0.5 * math.log2(math.e)

    def attend(g):
        first, count = groups[g]
        pool = pools[g]

        @pl.loop(0, count)
        def _(h):
            local = pl.ds(pl.multiple_of(h * HEAD_DIM, HEAD_DIM), HEAD_DIM)
            cols = pl.ds(pl.multiple_of((first + h) * HEAD_DIM, HEAD_DIM), HEAD_DIM)
            for step in range(tiles_dev):
                mine = step >= half_tiles
                side = half if mine else 1 - half
                tile = side * half_tiles + step % half_tiles
                query = query_ref[pl.ds(pl.multiple_of(tile * TILE, TILE), TILE), cols]
                slots = [slots_ref[tile * picks + p] for p in range(picks)]
                keys = jnp.concatenate([pool[s, 0, :, local] for s in slots], axis=0)
                values = jnp.concatenate([pool[s, 1, :, local] for s in slots], axis=0)
                scores = lax.dot_general(
                    query, keys, (((1,), (1,)), ((), ())), preferred_element_type=jnp.float32
                )
                parts = [
                    scores[:, p * TILE : (p + 1) * TILE] + bias_ref[tile * picks + p]
                    for p in range(picks)
                ]
                top = jnp.max(functools.reduce(jnp.maximum, parts), axis=1, keepdims=True)
                weights = [jnp.exp2((part - top) * factor) for part in parts]
                total = jnp.sum(functools.reduce(jnp.add, weights), axis=1, keepdims=True)
                rounded = jnp.concatenate([w.astype(jnp.bfloat16) for w in weights], axis=1)
                mixed = jnp.dot(rounded, values, preferred_element_type=jnp.float32)
                target = own if mine else away
                start = step % half_tiles * TILE
                target[start : start + TILE, cols] = (mixed / total).astype(jnp.bfloat16)

    def combine(g):
        first, count = groups[g]
        swap(g).wait_recv()
        cols = slice(first * HEAD_DIM, (first + count) * HEAD_DIM)
        mine = own[:, cols].astype(jnp.float32)
        from_other = theirs[:, cols].astype(jnp.float32)
        cond = jnp.where(half == 0, mine, from_other)
        uncond = jnp.where(half == 0, from_other, mine)
        out_ref[:, cols] = (uncond + guide_ref[0] * (cond - uncond)).astype(jnp.bfloat16)

    for g in range(len(groups)):
        for k, offset in enumerate(OFFSETS):

            @pl.when(inside(-offset))
            def _(k=k):
                route(g, k).wait_recv()

        attend(g)
        swap(g).start()
        if g > 0:
            combine(g - 1)
    for g in range(len(groups)):
        for k, offset in enumerate(OFFSETS):

            @pl.when(inside(offset))
            def _(k=k):
                route(g, k).wait_send()

        swap(g).wait_send()
    combine(len(groups) - 1)


def smem_spec():
    return pl.BlockSpec(memory_space=SMEM)


def head_groups(heads):
    shares = GROUP_SHARES if heads == sum(GROUP_SHARES) else (heads,)
    groups, first = [], 0
    for share in shares:
        groups.append((first, share))
        first += share
    return groups


def body(query_rows, key_rows, value_rows, select, counts, guide_scale):
    shards = lax.axis_size("seq") // 2
    index = lax.axis_index("seq")
    place = (index // 2).astype(jnp.int32).reshape(1)
    tokens, width = query_rows.shape
    tiles_dev = tokens // TILE
    picks = select.shape[1]
    half_rows = tokens // 2
    pool = tiles_dev + CAP * len(OFFSETS)

    send, slots, bias = pl.pallas_call(
        functools.partial(meta_kernel, shards, tiles_dev),
        out_shape=(
            jax.ShapeDtypeStruct((CAP * len(OFFSETS),), jnp.int32),
            jax.ShapeDtypeStruct((tiles_dev * picks,), jnp.int32),
            jax.ShapeDtypeStruct((tiles_dev * picks,), jnp.float32),
        ),
        in_specs=[smem_spec()] * 3,
        out_specs=(smem_spec(),) * 3,
        name="meta",
    )(place, select, counts)

    groups = head_groups(width // HEAD_DIM)
    whole = pl.BlockSpec(memory_space=pltpu.VMEM)
    rows = jnp.bfloat16
    copies = (len(groups), len(OFFSETS))
    return pl.pallas_call(
        functools.partial(main_kernel, groups, tiles_dev, picks),
        out_shape=jax.ShapeDtypeStruct((half_rows, width), rows),
        in_specs=[smem_spec()] * 4 + [whole] * 3,
        out_specs=whole,
        scratch_shapes=[pltpu.VMEM((pool, 2, TILE, n * HEAD_DIM), rows) for _, n in groups]
        + [pltpu.VMEM((len(OFFSETS), CAP, 2, TILE, n * HEAD_DIM), rows) for _, n in groups]
        + [pltpu.VMEM((half_rows, width), rows)] * 3
        + [pltpu.SemaphoreType.DMA(copies)] * 2
        + [pltpu.SemaphoreType.DMA((len(groups),))] * 2,
        compiler_params=pltpu.CompilerParams(
            collective_id=0, has_side_effects=True, vmem_limit_bytes=60000 * 1024
        ),
        name="main",
    )(
        send,
        slots,
        bias,
        guide_scale,
        query_rows,
        key_rows.reshape(tiles_dev, TILE, width),
        value_rows.reshape(tiles_dev, TILE, width),
    )


def solution(mesh):
    in_specs = (
        P(("groups", "seq"), None),
        P(("groups", "seq"), None),
        P(("groups", "seq"), None),
        P("groups", None),
        P("groups"),
        P("groups"),
    )
    out_specs = P(("groups", "seq"), None)
    return jax.shard_map(body, mesh=mesh, in_specs=in_specs, out_specs=out_specs, check_vma=False)
```

```python
import functools
import math

import jax
import jax.numpy as jnp
from jax import lax
from jax.experimental import pallas as pl
from jax.experimental.pallas import tpu as pltpu
from jax.sharding import PartitionSpec as P

HEAD_DIM = 128
TILE = 128
REACH = 2
CAP = 2
OFFSETS = (-1, 1, -2, 2)
GROUP_SHARES = (4, 4, 2, 1, 1)

SMEM = pltpu.SMEM


def wanted_span(select_ref, counts_ref, query_shard, owner_shard, shards, tiles_dev):
    first_row = jnp.clip(query_shard, 0, shards - 1) * tiles_dev
    low, high = jnp.int32(tiles_dev), jnp.int32(-1)
    for row in range(tiles_dev):
        count = counts_ref[first_row + row]
        for pick in range(select_ref.shape[0]):
            local = select_ref[pick, first_row + row] - owner_shard * tiles_dev
            usable = (local >= 0) & (local < tiles_dev) & (pick < count)
            low = jnp.where(usable, jnp.minimum(low, local), low)
            high = jnp.where(usable, jnp.maximum(high, local), high)
    low = jnp.where(high < 0, 0, low)
    return low, jnp.maximum(high, 0)


def meta_kernel(shards, tiles_dev, place_ref, select_ref, counts_ref, send_ref, slots_ref, bias_ref):
    shard = place_ref[0]
    picks = select_ref.shape[0]
    lows = []
    for k, offset in enumerate(OFFSETS):
        low, high = wanted_span(
            select_ref, counts_ref, shard + offset, shard, shards, tiles_dev
        )
        send_ref[CAP * k] = low
        send_ref[CAP * k + 1] = high
        lows.append(
            wanted_span(select_ref, counts_ref, shard, shard - offset, shards, tiles_dev)[0]
        )
    for row in range(tiles_dev):
        count = counts_ref[shard * tiles_dev + row]
        for pick in range(picks):
            local = select_ref[pick, shard * tiles_dev + row] - shard * tiles_dev
            slot = jnp.where((local >= 0) & (local < tiles_dev), local, 0)
            for k, offset in enumerate(OFFSETS):
                away = local + offset * tiles_dev
                there = (away >= 0) & (away < tiles_dev)
                second = jnp.where(away == lows[k], 0, 1)
                slot = jnp.where(there, tiles_dev + CAP * k + second, slot)
            slots_ref[row * picks + pick] = slot
            bias_ref[row * picks + pick] = jnp.where(pick < count, 0.0, -jnp.inf)


def main_kernel(groups, tiles_dev, picks, send_ref, slots_ref, bias_ref, guide_ref, *refs):
    query_ref, key_ref, value_ref, out_ref = refs[:4]
    refs = refs[4:]
    pools, outgoing = refs[: len(groups)], refs[len(groups) : 2 * len(groups)]
    own, away, theirs, send_sem, recv_sem, swap_send, swap_recv = refs[2 * len(groups) :]
    index = lax.axis_index("seq")
    shard, half = index // 2, index % 2
    shards = lax.axis_size("seq") // 2
    half_tiles = tiles_dev // 2
    other = index + 1 - 2 * half

    def inside(offset):
        return (shard + offset >= 0) & (shard + offset < shards)

    def route(g, k):
        return pltpu.make_async_remote_copy(
            src_ref=outgoing[g].at[k],
            dst_ref=pools[g].at[pl.ds(tiles_dev + CAP * k, CAP)],
            send_sem=send_sem.at[g, k],
            recv_sem=recv_sem.at[g, k],
            device_id={"seq": index + 2 * OFFSETS[k]},
            device_id_type=pl.DeviceIdType.MESH,
        )

    def swap(g):
        first, count = groups[g]
        cols = pl.ds(first * HEAD_DIM, count * HEAD_DIM)
        return pltpu.make_async_remote_copy(
            src_ref=away.at[:, cols],
            dst_ref=theirs.at[:, cols],
            send_sem=swap_send.at[g],
            recv_sem=swap_recv.at[g],
            device_id={"seq": other},
            device_id_type=pl.DeviceIdType.MESH,
        )

    barrier = pltpu.get_barrier_semaphore()
    pl.semaphore_signal(
        barrier, inc=1, device_id={"seq": other}, device_id_type=pl.DeviceIdType.MESH
    )
    greeted = jnp.int32(1)
    for offset in OFFSETS:
        greeted = greeted + jnp.where(inside(offset), 1, 0)

        @pl.when(inside(offset))
        def _(offset=offset):
            pl.semaphore_signal(
                barrier,
                inc=1,
                device_id={"seq": index + 2 * offset},
                device_id_type=pl.DeviceIdType.MESH,
            )

    def gather(g):
        first, count = groups[g]
        cols = slice(first * HEAD_DIM, (first + count) * HEAD_DIM)
        for k in range(len(OFFSETS)):
            for slot in range(CAP):
                tile = send_ref[CAP * k + slot]
                outgoing[g][k, slot, 0] = key_ref[tile, :, cols]
                outgoing[g][k, slot, 1] = value_ref[tile, :, cols]

    def launch(g):
        for k, offset in enumerate(OFFSETS):

            @pl.when(inside(offset))
            def _(k=k):
                route(g, k).start()

    gather(0)
    pl.semaphore_wait(barrier, greeted)
    for g in range(1, len(groups)):
        gather(g)
        launch(g - 1)
    for g, (first, count) in enumerate(groups):
        cols = slice(first * HEAD_DIM, (first + count) * HEAD_DIM)
        for tile in range(tiles_dev):
            pools[g][tile, 0] = key_ref[tile, :, cols]
            pools[g][tile, 1] = value_ref[tile, :, cols]
        if g == 0:
            launch(len(groups) - 1)

    factor = HEAD_DIM**-0.5 * math.log2(math.e)

    def attend(g, steps):
        first, count = groups[g]
        pool = pools[g]

        @pl.loop(0, count)
        def _(h):
            local = pl.ds(pl.multiple_of(h * HEAD_DIM, HEAD_DIM), HEAD_DIM)
            cols = pl.ds(pl.multiple_of((first + h) * HEAD_DIM, HEAD_DIM), HEAD_DIM)
            for step in steps:
                mine = step >= half_tiles
                side = half if mine else 1 - half
                tile = side * half_tiles + step % half_tiles
                query = query_ref[pl.ds(pl.multiple_of(tile * TILE, TILE), TILE), cols]
                slots = [slots_ref[tile * picks + p] for p in range(picks)]
                keys = jnp.concatenate([pool[s, 0, :, local] for s in slots], axis=0)
                values = jnp.concatenate([pool[s, 1, :, local] for s in slots], axis=0)
                scores = lax.dot_general(
                    query, keys, (((1,), (1,)), ((), ())), preferred_element_type=jnp.float32
                )
                parts = [
                    scores[:, p * TILE : (p + 1) * TILE] + bias_ref[tile * picks + p]
                    for p in range(picks)
                ]
                top = jnp.max(functools.reduce(jnp.maximum, parts), axis=1, keepdims=True)
                weights = [jnp.exp2((part - top) * factor) for part in parts]
                total = jnp.sum(functools.reduce(jnp.add, weights), axis=1, keepdims=True)
                rounded = jnp.concatenate([w.astype(jnp.bfloat16) for w in weights], axis=1)
                mixed = jnp.dot(rounded, values, preferred_element_type=jnp.float32)
                target = own if mine else away
                start = step % half_tiles * TILE
                target[start : start + TILE, cols] = (mixed / total).astype(jnp.bfloat16)

    def combine(g):
        first, count = groups[g]
        swap(g).wait_recv()
        cols = slice(first * HEAD_DIM, (first + count) * HEAD_DIM)
        mine = own[:, cols].astype(jnp.float32)
        from_other = theirs[:, cols].astype(jnp.float32)
        cond = jnp.where(half == 0, mine, from_other)
        uncond = jnp.where(half == 0, from_other, mine)
        out_ref[:, cols] = (uncond + guide_ref[0] * (cond - uncond)).astype(jnp.bfloat16)

    for g in range(len(groups)):
        for k, offset in enumerate(OFFSETS):

            @pl.when(inside(-offset))
            def _(k=k):
                route(g, k).wait_recv()

        if g < len(groups) - 1:
            attend(g, range(tiles_dev))
            swap(g).start()
        else:
            attend(g, range(half_tiles))
            swap(g).start()
            attend(g, range(half_tiles, tiles_dev))
        if g > 0:
            combine(g - 1)
    for g in range(len(groups)):
        for k, offset in enumerate(OFFSETS):

            @pl.when(inside(offset))
            def _(k=k):
                route(g, k).wait_send()

        swap(g).wait_send()
    combine(len(groups) - 1)


def smem_spec():
    return pl.BlockSpec(memory_space=SMEM)


def head_groups(heads):
    shares = GROUP_SHARES if heads == sum(GROUP_SHARES) else (heads,)
    groups, first = [], 0
    for share in shares:
        groups.append((first, share))
        first += share
    return groups


def body(query_rows, key_rows, value_rows, select, counts, guide_scale):
    shards = lax.axis_size("seq") // 2
    index = lax.axis_index("seq")
    place = (index // 2).astype(jnp.int32).reshape(1)
    tokens, width = query_rows.shape
    tiles_dev = tokens // TILE
    picks = select.shape[1]
    half_rows = tokens // 2
    pool = tiles_dev + CAP * len(OFFSETS)

    send, slots, bias = pl.pallas_call(
        functools.partial(meta_kernel, shards, tiles_dev),
        out_shape=(
            jax.ShapeDtypeStruct((CAP * len(OFFSETS),), jnp.int32),
            jax.ShapeDtypeStruct((tiles_dev * picks,), jnp.int32),
            jax.ShapeDtypeStruct((tiles_dev * picks,), jnp.float32),
        ),
        in_specs=[smem_spec()] * 3,
        out_specs=(smem_spec(),) * 3,
        name="meta",
    )(place, select.T, counts)

    groups = head_groups(width // HEAD_DIM)
    whole = pl.BlockSpec(memory_space=pltpu.VMEM)
    rows = jnp.bfloat16
    copies = (len(groups), len(OFFSETS))
    return pl.pallas_call(
        functools.partial(main_kernel, groups, tiles_dev, picks),
        out_shape=jax.ShapeDtypeStruct((half_rows, width), rows),
        in_specs=[smem_spec()] * 4 + [whole] * 3,
        out_specs=whole,
        scratch_shapes=[pltpu.VMEM((pool, 2, TILE, n * HEAD_DIM), rows) for _, n in groups]
        + [pltpu.VMEM((len(OFFSETS), CAP, 2, TILE, n * HEAD_DIM), rows) for _, n in groups]
        + [pltpu.VMEM((half_rows, width), rows)] * 3
        + [pltpu.SemaphoreType.DMA(copies)] * 2
        + [pltpu.SemaphoreType.DMA((len(groups),))] * 2,
        compiler_params=pltpu.CompilerParams(
            collective_id=0, has_side_effects=True, vmem_limit_bytes=60000 * 1024
        ),
        name="main",
    )(
        send,
        slots,
        bias,
        guide_scale,
        query_rows,
        key_rows.reshape(tiles_dev, TILE, width),
        value_rows.reshape(tiles_dev, TILE, width),
    )


def solution(mesh):
    in_specs = (
        P(("groups", "seq"), None),
        P(("groups", "seq"), None),
        P(("groups", "seq"), None),
        P("groups", None),
        P("groups"),
        P("groups"),
    )
    out_specs = P(("groups", "seq"), None)
    return jax.shard_map(body, mesh=mesh, in_specs=in_specs, out_specs=out_specs, check_vma=False)
```
